1024 devices in a mesh: node: 32 (over z, core), dev: 32 (over y, x).
Axes of the slice: x: 4, y: 8, z: 16, core: 2. Of those that a mesh axis runs over, the one named last changes fastest.
Arguments:
- blocks: bfloat16 [32, 32, 16, 7, 16, 256], P('node', 'dev'), may hold values from -6 to 6
- levels: int32 [32, 32, 16], P('node', 'dev'), may hold values from 0 to 3
- destinations: int32 [32, 32, 16], P('node', 'dev'), may hold values from 0 to 31, as said below
- speeds: float32 [7], replicated, may hold values from -1 to 1
- thresholds: float32 [7], replicated, may hold values from 0.1 to 1
Outputs:
- updated: bfloat16 [32, 32, 32, 7, 16, 256], P('node', 'dev')
- new_levels: int32 [32, 32, 32], P('node', 'dev')
The draws below stay inside these ranges and needn't reach their ends.
Inputs may be any that keep to these rules, and one draw needn't show every extreme that they name: `destinations`: at most 1 block of one device go to one device, and at most 32 blocks arrive at one device; in every group both bounds are reached.
All inputs are finite; a program needn't handle non-finite values.
Results may differ from the reference program's by a relative error of at most 0.001.
Values may be sent and summed in bfloat16 or wider, within the bound.
No kernel may reach another device: no remote copies, remote signals or barrier semaphores. Data moves between devices by JAX's collectives and lax.ppermute only.
A program may use at most 32 MiB of HBM per device.

```python
import math
import jax
import jax.numpy as jnp
from jax import lax

QUANT = 7
EDGE = 16
LEVELS = 4
SLOTS = 16
GROUPS = 32
OWNERS = 32
NEW_CAP = 32


def draw_destinations(key, part):

    def one_group(group_key):
        rank_key, label_key, slot_key = jax.random.split(group_key, 3)
        sender_rank = jax.random.permutation(rank_key, OWNERS).astype(jnp.int32)
        labels = jax.random.permutation(label_key, OWNERS).astype(jnp.int32)
        slot_order = jax.vmap(lambda single_key: jax.random.permutation(single_key, SLOTS))(jax.random.split(slot_key, OWNERS)).astype(jnp.int32)
        serial = slot_order * OWNERS + sender_rank[:, None]
        others = 1 + jnp.mod(serial - 2 * SLOTS, OWNERS - 1)
        picked = jnp.where(serial < 2 * SLOTS, 0, others)
        return labels[picked].astype(jnp.int32)
    return jax.vmap(one_group)(jax.random.split(jax.random.fold_in(key, 17), GROUPS))


def place_ends(values, stream_key, smallest, high):
    longest = values.shape.index(max(values.shape))
    spots = []
    for shift in (0, 1):
        where = [jax.random.randint(jax.random.fold_in(stream_key, axis), (), 0, length) for axis, length in enumerate(values.shape)]
        where[longest] = (where[longest] + shift) % values.shape[longest]
        spots.append(tuple(where))
    return values.at[spots[0]].set(smallest).at[spots[1]].set(high)


def level_of(stream_key, extent, cuts, low, top_value):
    level = 1.0
    for dim, shards_of in cuts:
        heights = jax.random.uniform(jax.random.fold_in(jax.random.fold_in(stream_key, 6), dim), (shards_of,), jnp.float32, low / len(cuts), top_value / len(cuts))
        level = level * jnp.repeat(jnp.exp(heights), extent[dim] // shards_of).reshape((-1,) + (1,) * (len(extent) - 1 - dim))
    return level


def gaussian(stream_key, extent, scale, most, pieces=(), held_as=jnp.bfloat16):
    values = scale * jax.random.normal(stream_key, extent, jnp.float32)
    if pieces:
        values = values * level_of(stream_key, extent, pieces, -0.22, 0.18)
    return jnp.clip(values, -most, most).astype(held_as)


def setup_inputs(seed: int = 0) -> dict:
    splits = jax.random.split(jax.random.key(seed), 6)
    return {
        "blocks": gaussian(splits[0], (GROUPS, OWNERS, SLOTS, QUANT, EDGE, EDGE * EDGE), 1.0, 6.0, ((0, 32), (1, 32))),
        "levels": place_ends(jax.random.randint(splits[1], (GROUPS, OWNERS, SLOTS), 0, LEVELS), jax.random.fold_in(splits[1], 1), 0, LEVELS - 1).astype(jnp.int32),
        "destinations": draw_destinations(jax.random.fold_in(splits[5], 71), 0),
        "speeds": jnp.clip(jax.random.uniform(splits[3], (QUANT,), jnp.float32, -1.0, 1.0), -1.0, 1.0),
        "thresholds": jnp.clip(jnp.exp(jax.random.uniform(splits[4], (QUANT,), jnp.float32, math.log(0.1), math.log(1.0))), 0.1, 1.0),
    }


COURANT = 0.4
WENO_EPS = 1e-6


def square(value):
    return value * value


def weno_face(first, second, third, fourth, fifth):
    guess_zero = (2.0 * first - 7.0 * second + 11.0 * third) / 6.0
    guess_one = (-second + 5.0 * third + 2.0 * fourth) / 6.0
    guess_two = (2.0 * third + 5.0 * fourth - fifth) / 6.0
    smooth_zero = 13.0 / 12.0 * square(first - 2.0 * second + third) + 0.25 * square(first - 4.0 * second + 3.0 * third)
    smooth_one = 13.0 / 12.0 * square(second - 2.0 * third + fourth) + 0.25 * square(second - fourth)
    smooth_two = 13.0 / 12.0 * square(third - 2.0 * fourth + fifth) + 0.25 * square(3.0 * third - 4.0 * fourth + fifth)
    weight_zero = 0.1 / square(WENO_EPS + smooth_zero)
    weight_one = 0.6 / square(WENO_EPS + smooth_one)
    weight_two = 0.3 / square(WENO_EPS + smooth_two)
    total = weight_zero + weight_one + weight_two
    return (weight_zero * guess_zero + weight_one * guess_one + weight_two * guess_two) / total


def shape_ghosts(near_layers, near_tag, own_tag):
    same_level = near_layers[:, :, 0:3]
    finer_level = 0.5 * (near_layers[:, :, 0:6:2] + near_layers[:, :, 1:6:2])
    coarser = jnp.concatenate([near_layers[:, :, 0:1], near_layers[:, :, 0:1], near_layers[:, :, 1:2]], axis=2)
    offset = jnp.clip(near_tag - own_tag, -1, 1)[:, None, None, None]
    ghost_cells = jnp.where(offset > 0, finer_level, jnp.where(offset < 0, coarser, same_level))
    return lax.optimization_barrier(ghost_cells.astype(jnp.bfloat16))


def advance_quantity(extended, occupied, velocity, threshold):
    cells = extended.shape[1] - 6
    stencil = [extended[:, k:k + cells + 1] for k in range(6)]
    left_state = weno_face(stencil[0], stencil[1], stencil[2], stencil[3], stencil[4])
    right_state = weno_face(stencil[5], stencil[4], stencil[3], stencil[2], stencil[1])
    fluxes = jnp.maximum(velocity, 0.0) * left_state + jnp.minimum(velocity, 0.0) * right_state
    advanced = extended[:, 3:3 + cells] - COURANT * (fluxes[:, 1:] - fluxes[:, :-1])
    even_cells = advanced[:, 0::2]
    odd_cells = advanced[:, 1::2]
    predicted = jnp.concatenate([0.5 * (even_cells[:, :-1] + even_cells[:, 1:]), even_cells[:, -1:]], axis=1)
    detail = odd_cells - predicted
    kept_cells = predicted + detail - jnp.clip(detail, -threshold, threshold)
    result = jnp.stack([even_cells, kept_cells], axis=2).reshape(advanced.shape)
    return jnp.where(occupied[:, None, None], result, 0.0).astype(jnp.bfloat16)


def reference(blocks, levels, destinations, speeds, thresholds):
    flat_targets = destinations.reshape(GROUPS, OWNERS * SLOTS)
    owner_ids = jnp.arange(OWNERS).astype(jnp.int32)
    matches = (flat_targets[:, :, None] == owner_ids[None, None, :]).astype(jnp.int32)
    earlier = jnp.cumsum(matches, axis=1) - matches
    position = jnp.sum(earlier * matches, axis=2)
    target_index = (flat_targets * NEW_CAP + position).astype(jnp.int32)
    group_index = jnp.arange(GROUPS).astype(jnp.int32)[:, None]
    arranged = jnp.zeros((GROUPS, OWNERS * NEW_CAP, QUANT, EDGE, EDGE * EDGE), blocks.dtype)
    arranged = arranged.at[group_index, target_index].set(blocks.reshape(GROUPS, OWNERS * SLOTS, QUANT, EDGE, EDGE * EDGE))
    block_tag = jnp.zeros((GROUPS, OWNERS * NEW_CAP), jnp.int32)
    block_tag = block_tag.at[group_index, target_index].set((levels.reshape(GROUPS, OWNERS * SLOTS) + 1).astype(jnp.int32))
    below = arranged[:, :, :, EDGE - 6:]
    lower_faces = jnp.concatenate([jnp.zeros_like(below[:1]), below[:-1]], axis=0)
    above = arranged[:, :, :, :6]
    upper_faces = jnp.concatenate([above[1:], jnp.zeros_like(above[:1])], axis=0)
    lower_tags = jnp.concatenate([jnp.zeros_like(block_tag[:1]), block_tag[:-1]], axis=0)
    upper_tags = jnp.concatenate([block_tag[1:], jnp.zeros_like(block_tag[:1])], axis=0)

    def one_group(member):
        own_blocks, own_tag, lower_layers, lower_tag, upper_layers, upper_tag = member
        ghost_low = shape_ghosts(lower_layers.astype(jnp.float32)[:, :, ::-1], lower_tag, own_tag)[:, :, ::-1]
        ghost_high = shape_ghosts(upper_layers.astype(jnp.float32), upper_tag, own_tag)
        extended = jnp.concatenate([ghost_low, own_blocks, ghost_high], axis=2).astype(jnp.float32)
        extended = jnp.moveaxis(extended, 1, 0)
        occupied = own_tag > 0
        result = lax.map(lambda entry: advance_quantity(entry[0], occupied, entry[1], entry[2]), (extended, speeds, thresholds))
        return jnp.moveaxis(result, 0, 1)

    updated = lax.map(one_group, (arranged, block_tag, lower_faces, lower_tags, upper_faces, upper_tags))
    updated = updated.reshape(GROUPS, OWNERS, NEW_CAP, QUANT, EDGE, EDGE * EDGE)
    new_levels = (block_tag - 1).reshape(GROUPS, OWNERS, NEW_CAP)
    return updated, new_levels
```

```python
import jax
import jax.numpy as jnp
from jax import lax
from jax.experimental import pallas as pl
from jax.experimental.pallas import tpu as pltpu
from jax.sharding import PartitionSpec as P

QUANT = 7
EDGE = 16
PLANE = EDGE * EDGE
SLOTS = 16
NEW_CAP = 32
LANES = 128
HALVES = PLANE // LANES
PITCH = EDGE + 1

COURANT = 0.4
WENO_EPS = 1e-06

SMEM = pl.BlockSpec(memory_space=pltpu.SMEM)
VMEM = pl.BlockSpec(memory_space=pltpu.VMEM)
ANY = pl.BlockSpec(memory_space=pl.ANY)


def label_kernel(dest_ref, level_ref, out_ref):
    row = lax.broadcasted_iota(jnp.int32, out_ref.shape, 0)
    tags = jnp.zeros(out_ref.shape, jnp.int32)
    for s in range(SLOTS):
        tags = jnp.where(row == dest_ref[0, 0, s], level_ref[0, 0, s] + 1, tags)
    out_ref[...] = tags


def pack_kernel(dest_ref, blocks_ref, out_ref, sems):
    copies = [
        pltpu.make_async_copy(blocks_ref.at[s], out_ref.at[dest_ref[0, 0, s]], sems.at[s])
        for s in range(SLOTS)
    ]
    for copy in copies:
        copy.start()
    for copy in copies:
        copy.wait()


def rank_kernel(tags_sm, tags_ref, source_ref, count_ref, new_ref, own_ref):
    own_ref[...] = jnp.zeros_like(own_ref)
    for p in range(NEW_CAP):
        source_ref[p] = 0
        new_ref[p] = -1
    count = jnp.int32(0)
    for i in range(NEW_CAP):
        tag = tags_sm[i, 0]
        here = tag > 0

        @pl.when(here)
        def _(i=i, tag=tag, count=count):
            source_ref[count] = i
            new_ref[count] = tag - 1
            own_ref[pl.ds(count, 1), :] = tags_ref[pl.ds(i, 1), :]

        count = count + here.astype(jnp.int32)
    count_ref[0] = count


def shaped(layers, finer, coarser):
    result = []
    for m in (1, 2, 3):
        same = layers[m - 1]
        fine = 0.5 * (layers[2 * m - 2] + layers[2 * m - 1])
        coarse = layers[(m + 1) // 2 - 1]
        result.append(jnp.where(finer, fine, jnp.where(coarser, coarse, same)))
    return result


def arrange_kernel(
    source_ref, count_ref, own_ref, low_ref, high_ref, in_ref, out_ref, below_ref, above_ref, work
):
    count = count_ref[0]
    own = own_ref[...]
    low = low_ref[...]
    high = high_ref[...]
    for half in range(HALVES):
        lanes = slice(half * LANES, (half + 1) * LANES)
        for p in range(NEW_CAP):
            cells = in_ref[source_ref[p], 0, :, lanes].astype(jnp.float32)
            work[half, p * PITCH : p * PITCH + EDGE, :] = jnp.where(p < count, cells, 0.0)
        layers = []
        for c in range(EDGE):
            layer = work[half, pl.ds(c, NEW_CAP, stride=PITCH), :]
            out_ref[0, c, :, lanes] = layer.astype(jnp.bfloat16)
            layers.append(layer)
            if c == 5:
                for m, ghost in enumerate(shaped(layers, own > low, own < low)):
                    below_ref[0, m, :, lanes] = ghost.astype(jnp.bfloat16)
        top = layers[: EDGE - 7 : -1]
        for m, ghost in enumerate(shaped(top, own > high, own < high)):
            above_ref[0, m, :, lanes] = ghost.astype(jnp.bfloat16)


def face_ratios(read):
    cells, steps, halves, wides, curves = [], [], [], [], []
    for k in range(EDGE + 6):
        cells.append(read(k))
        if k >= 1:
            step = cells[k] - cells[k - 1]
            half = 0.5 * step
            steps.append(step)
            halves.append(half)
            wides.append(step + half)
        if k >= 2:
            bend = steps[k - 1] - steps[k - 2]
            curves.append((13.0 / 12.0) * (bend * bend) + WENO_EPS)
        if k >= 4:
            f = k - 4
            one = wides[f + 1] - halves[f]
            two = halves[f + 1] + halves[f + 2]
            three = wides[f + 2] - halves[f + 3]
            p_zero = curves[f] + one * one
            p_one = curves[f + 1] + two * two
            p_two = curves[f + 2] + three * three
            w_zero = p_one * p_two
            w_one = p_zero * p_two
            w_two = p_zero * p_one
            w_zero = w_zero * w_zero
            w_one = 6.0 * (w_one * w_one)
            w_two = 3.0 * (w_two * w_two)
            g_zero = 2.5 * steps[f + 1] - steps[f]
            g_one = halves[f + 1] + steps[f + 2]
            g_two = 2.0 * steps[f + 2] - halves[f + 3]
            total = w_zero + w_one + w_two
            ratio = (w_zero * g_zero + w_one * g_one + w_two * g_two) / total
            yield cells[f + 2], ratio


def advance_kernel(
    speed_ref, limit_ref, count_ref, in_ref, low_ref, high_ref, out_ref, work
):
    count = count_ref[0]
    q = pl.program_id(0)
    speed = speed_ref[q]
    limit = limit_ref[q]
    rate = COURANT * jnp.abs(speed)
    third = rate / 3.0
    group = 16

    def run(forward):
        def tile(index, carry):
            half = index % HALVES
            base = pl.multiple_of((index // HALVES) * group, group)
            lanes = pl.ds(pl.multiple_of(half * LANES, LANES), LANES)
            rows = pl.ds(base, group)

            def read(k):
                k = k if forward else EDGE + 5 - k
                if k < 3:
                    part = low_ref[0, 2 - k, rows, lanes]
                elif k < EDGE + 3:
                    part = in_ref[0, k - 3, rows, lanes]
                else:
                    part = high_ref[0, k - EDGE - 3, rows, lanes]
                return part.astype(jnp.float32)

            advanced = {}

            def emit(c):
                slot = work.at[pl.ds(c, group, stride=PITCH), :]
                if c % 2 == 0:
                    slot[...] = advanced[c]
                    return
                if c == EDGE - 1:
                    guess = advanced[c - 1]
                else:
                    guess = 0.5 * (advanced[c - 1] + advanced[c + 1])
                detail = advanced[c] - guess
                slot[...] = guess + detail - jnp.clip(detail, -limit, limit)

            last = None
            for f, (centre, ratio) in enumerate(face_ratios(read)):
                flux = rate * centre + third * ratio
                if f >= 1:
                    k = f - 1
                    c = k if forward else EDGE - 1 - k
                    advanced[c] = read(k + 3) - (flux - last)
                    if c % 2 == 0:
                        emit(c)
                        if forward and c >= 2:
                            emit(c - 1)
                        if not forward:
                            emit(c + 1)
                last = flux
            if forward:
                emit(EDGE - 1)
            for p in range(group):
                cells = work[p * PITCH : p * PITCH + EDGE, :]
                cells = jnp.where(base + p < count, cells, 0.0)
                out_ref[base + p, 0, :, lanes] = cells.astype(jnp.bfloat16)
            return carry

        lax.fori_loop(0, HALVES * (NEW_CAP // group), tile, 0)

    @pl.when(speed >= 0.0)
    def _():
        run(True)

    @pl.when(speed < 0.0)
    def _():
        run(False)


def struct(shape, dtype):
    return jax.ShapeDtypeStruct(shape, dtype)


def body(blocks, levels, destinations, speeds, thresholds):
    owners = lax.axis_size("dev")
    count = lax.axis_size("node")
    up = [(i, i + 1) for i in range(count - 1)]
    down = [(i + 1, i) for i in range(count - 1)]
    labels = pl.pallas_call(
        label_kernel,
        in_specs=[SMEM, SMEM],
        out_specs=VMEM,
        out_shape=struct((owners, LANES), jnp.int32),
        name="label",
    )(destinations, levels)
    labels = lax.all_to_all(
        labels.reshape(owners, 1, LANES), "dev", split_axis=0, concat_axis=0, tiled=True
    ).reshape(owners, LANES)
    outgoing = pl.pallas_call(
        pack_kernel,
        in_specs=[SMEM, VMEM],
        out_specs=ANY,
        out_shape=struct((owners, QUANT, EDGE, PLANE), jnp.bfloat16),
        scratch_shapes=[pltpu.SemaphoreType.DMA((SLOTS,))],
        name="pack",
    )(destinations, blocks.reshape(SLOTS, QUANT, EDGE, PLANE))
    incoming = lax.all_to_all(outgoing, "dev", split_axis=0, concat_axis=0, tiled=True)
    source, total, new_levels, own = pl.pallas_call(
        rank_kernel,
        in_specs=[SMEM, VMEM],
        out_specs=(SMEM, SMEM, SMEM, VMEM),
        out_shape=(
            struct((NEW_CAP,), jnp.int32),
            struct((1,), jnp.int32),
            struct((NEW_CAP,), jnp.int32),
            struct((NEW_CAP, LANES), jnp.int32),
        ),
        name="rank",
    )(labels, labels)
    low_tag = lax.ppermute(own, "node", up)
    high_tag = lax.ppermute(own, "node", down)
    plane = (1, EDGE, NEW_CAP, PLANE)
    ghost = (1, 3, NEW_CAP, PLANE)
    natural = (NEW_CAP, 1, EDGE, PLANE)
    by_quantity = lambda q: (q, 0, 0, 0)
    arranged, for_below, for_above = pl.pallas_call(
        arrange_kernel,
        grid=(QUANT,),
        in_specs=[
            SMEM,
            SMEM,
            VMEM,
            VMEM,
            VMEM,
            pl.BlockSpec(natural, lambda q: (0, q, 0, 0)),
        ],
        out_specs=(
            pl.BlockSpec(plane, by_quantity),
            pl.BlockSpec(ghost, by_quantity),
            pl.BlockSpec(ghost, by_quantity),
        ),
        out_shape=(
            struct((QUANT, EDGE, NEW_CAP, PLANE), jnp.bfloat16),
            struct((QUANT, 3, NEW_CAP, PLANE), jnp.bfloat16),
            struct((QUANT, 3, NEW_CAP, PLANE), jnp.bfloat16),
        ),
        scratch_shapes=[pltpu.VMEM((HALVES, NEW_CAP * PITCH + 8, LANES), jnp.float32)],
        name="arrange",
    )(source, total, own, low_tag, high_tag, incoming)
    ghost_high = lax.ppermute(for_below, "node", down)
    ghost_low = lax.ppermute(for_above, "node", up)
    updated = pl.pallas_call(
        advance_kernel,
        grid=(QUANT,),
        in_specs=[
            SMEM,
            SMEM,
            SMEM,
            pl.BlockSpec(plane, by_quantity),
            pl.BlockSpec(ghost, by_quantity),
            pl.BlockSpec(ghost, by_quantity),
        ],
        out_specs=pl.BlockSpec(natural, lambda q: (0, q, 0, 0)),
        out_shape=struct((NEW_CAP, QUANT, EDGE, PLANE), jnp.bfloat16),
        scratch_shapes=[pltpu.VMEM((16 * PITCH + 8, LANES), jnp.float32)],
        name="advance",
    )(speeds, thresholds, total, arranged, ghost_low, ghost_high)
    return (
        updated.reshape(1, 1, NEW_CAP, QUANT, EDGE, PLANE),
        new_levels.reshape(1, 1, NEW_CAP),
    )


def solution(mesh):
    return jax.shard_map(
        body,
        mesh=mesh,
        in_specs=(
            P("node", "dev", None, None, None, None),
            P("node", "dev", None),
            P("node", "dev", None),
            P(),
            P(),
        ),
        out_specs=(P("node", "dev", None, None, None, None), P("node", "dev", None)),
        check_vma=False,
    )
```

```python
import jax
import jax.numpy as jnp
from jax import lax
from jax.experimental import pallas as pl
from jax.experimental.pallas import tpu as pltpu
from jax.sharding import PartitionSpec as P

QUANT = 7
EDGE = 16
PLANE = EDGE * EDGE
SLOTS = 16
NEW_CAP = 32
LANES = 128
HALVES = PLANE // LANES
PITCH = EDGE + 1
GROUP = 16
HALF_TILES = QUANT * EDGE // 8
ROW_TILES = HALVES * HALF_TILES + 1
SENT = 5

COURANT = 0.4
WENO_EPS = 1e-06

SMEM = pl.BlockSpec(memory_space=pltpu.SMEM)
VMEM = pl.BlockSpec(memory_space=pltpu.VMEM)
ANY = pl.BlockSpec(memory_space=pl.ANY)


def pack_kernel(
    dest_ref, level_ref, blocks_ref, out_ref, work, tags, in_sems, out_sems, tag_sem
):
    loads = [
        pltpu.make_async_copy(blocks_ref.at[s], work.at[s], in_sems.at[s]) for s in range(SLOTS)
    ]
    for load in loads:
        load.start()
    row = lax.broadcasted_iota(jnp.int32, tags.shape, 0)
    values = jnp.zeros(tags.shape, jnp.int32)
    for s in range(SLOTS):
        values = jnp.where(row == dest_ref[0, 0, s], level_ref[0, 0, s] + 1, values)
    tags[...] = values.astype(jnp.float32).astype(jnp.bfloat16)
    stores = [pltpu.make_async_copy(tags, out_ref.at[:, ROW_TILES - 1], tag_sem)]
    stores[0].start()
    for s in range(SLOTS):
        loads[s].wait()
        for half in range(HALVES):
            store = pltpu.make_async_copy(
                work.at[s, :, :, half * LANES : (half + 1) * LANES],
                out_ref.at[dest_ref[0, 0, s], half * HALF_TILES : (half + 1) * HALF_TILES],
                out_sems.at[s, half],
            )
            store.start()
            stores.append(store)
    for store in stores:
        store.wait()


def rank_positions(in_ref, source, count_ref, new_ref, own_ref, tags_vm, tags_sm, sem):
    for i in range(NEW_CAP):
        tile = in_ref[i, ROW_TILES - 1].astype(jnp.float32)
        tags_vm[i : i + 1, :] = tile[0:1].astype(jnp.int32)
    copy = pltpu.make_async_copy(tags_vm, tags_sm, sem)
    copy.start()
    own_ref[...] = jnp.zeros_like(own_ref)
    for p in range(NEW_CAP):
        source[p] = 0
        new_ref[p] = -1
    copy.wait()
    count = jnp.int32(0)
    for i in range(NEW_CAP):
        tag = tags_sm[i, 0]
        here = tag > 0

        @pl.when(here)
        def _(i=i, tag=tag, count=count):
            source[count] = i
            new_ref[count] = tag - 1
            own_ref[pl.ds(count, 1), :] = tags_vm[pl.ds(i, 1), :]

        count = count + here.astype(jnp.int32)
    count_ref[0] = count
    return count


def arrange_kernel(
    in_ref, out_ref, below_ref, above_ref, own_ref, count_ref, new_ref,
    work, source, tags_vm, tags_sm, sem,
):
    count = rank_positions(in_ref, source, count_ref, new_ref, own_ref, tags_vm, tags_sm, sem)

    def quantity(q, carry):
        for half in range(HALVES):
            lanes = slice(half * LANES, (half + 1) * LANES)
            for p in range(NEW_CAP):
                for part in range(2):
                    tile = half * HALF_TILES + 2 * q + part
                    cells = in_ref[source[p], tile].astype(jnp.float32)
                    start = p * PITCH + part * 8
                    work[half, start : start + 8, :] = jnp.where(p < count, cells, 0.0)
            layers = []
            for c in range(EDGE):
                layer = work[half, pl.ds(c, NEW_CAP, stride=PITCH), :]
                out_ref[q, c, :, lanes] = layer.astype(jnp.bfloat16)
                layers.append(layer)
            for ref, near_layers in ((below_ref, layers), (above_ref, layers[::-1])):
                sent = list(near_layers[:3])
                sent.append(0.5 * (near_layers[2] + near_layers[3]))
                sent.append(0.5 * (near_layers[4] + near_layers[5]))
                for m, layer in enumerate(sent):
                    ref[SENT * q + m, :, lanes] = layer.astype(jnp.bfloat16)
        return carry

    lax.fori_loop(0, QUANT, quantity, 0)
    label = own_ref[...].astype(jnp.float32).astype(jnp.bfloat16)
    for half in range(HALVES):
        lanes = slice(half * LANES, (half + 1) * LANES)
        below_ref[SENT * QUANT, :, lanes] = label
        above_ref[SENT * QUANT, :, lanes] = label


def faces(read, first, last):
    cells, steps, bends, curves, turns = {}, {}, {}, {}, {}
    for k in range(first, last + 5):
        cells[k] = read(k)
        if k >= first + 1:
            steps[k] = cells[k] - cells[k - 1]
        if k >= first + 2:
            bends[k - 1] = 0.5 * (steps[k] - steps[k - 1])
            curves[k - 1] = (13.0 / 3.0) * (bends[k - 1] * bends[k - 1]) + WENO_EPS
        if k >= first + 3:
            turns[k - 1] = bends[k - 2] - bends[k - 1]
        if k >= first + 4:
            c = k - 2
            one = steps[c] + bends[c - 1]
            two = steps[c] + bends[c]
            three = steps[c + 1] - bends[c + 1]
            p_zero = curves[c - 1] + one * one
            p_one = curves[c] + two * two
            p_two = curves[c + 1] + three * three
            w_zero = p_one * p_two
            w_one = p_zero * p_two
            w_two = p_zero * p_one
            w_zero = w_zero * w_zero
            w_one = w_one * w_one
            w_two = 1.5 * (w_two * w_two)
            total = (w_zero + 6.0 * w_one) + (w_two + w_two)
            shift = (w_zero * turns[c] + w_two * turns[c + 1]) / total
            yield k - 4, 0.75 * (cells[c] + cells[c + 1]) + (shift - 0.5 * bends[c])


def tiles(body_of):
    def tile(index, carry):
        half = index % HALVES
        base = pl.multiple_of((index // HALVES) * GROUP, GROUP)
        body_of(base, pl.ds(base, GROUP), pl.ds(pl.multiple_of(half * LANES, LANES), LANES))
        return carry

    lax.fori_loop(0, HALVES * (NEW_CAP // GROUP), tile, 0)


def by_direction(speed_ref, q, run):
    @pl.when(speed_ref[q] >= 0.0)
    def _():
        run(q, True)

    @pl.when(speed_ref[q] < 0.0)
    def _():
        run(q, False)


def inner_kernel(speed_ref, in_ref, mid_ref):
    def run(q, forward):
        rate = (COURANT * 2.0 / 3.0) * jnp.abs(speed_ref[q])

        def tile(base, rows, lanes):
            def read(k):
                c = k - 3 if forward else EDGE + 2 - k
                return in_ref[q, c, rows, lanes].astype(jnp.float32)

            last = None
            for f, state in faces(read, 3, EDGE - 2):
                if f == 3:
                    mid_ref[q, 0, rows, lanes] = state
                else:
                    mid_ref[q, f - 3, rows, lanes] = read(f + 2) - rate * (state - last)
                last = state
            mid_ref[q, EDGE - 4, rows, lanes] = last

        tiles(tile)

    def quantity(q, carry):
        by_direction(speed_ref, q, run)
        return carry

    lax.fori_loop(0, QUANT, quantity, 0)


def outer_kernel(
    speed_ref, limit_ref, count_ref, own_ref, in_ref, mid_ref, low_ref, high_ref, out_ref,
    done, work, sems,
):
    count = count_ref[0]

    def run(q, forward):
        limit = limit_ref[q]
        rate = (COURANT * 2.0 / 3.0) * jnp.abs(speed_ref[q])

        def tile(base, rows, lanes):
            own = own_ref[rows, :].astype(jnp.float32)

            def ghosts(ref):
                sent = [
                    ref[SENT * q + m, rows, lanes].astype(jnp.float32) for m in range(SENT)
                ]
                mean = (0.5 * (sent[0] + sent[1])).astype(jnp.bfloat16).astype(jnp.float32)
                tag = ref[SENT * QUANT, rows, lanes].astype(jnp.float32)
                finer = tag > own
                coarser = tag < own
                return [
                    jnp.where(finer, fine, jnp.where(coarser, coarse, same))
                    for fine, coarse, same in (
                        (mean, sent[0], sent[0]),
                        (sent[3], sent[0], sent[1]),
                        (sent[4], sent[1], sent[2]),
                    )
                ]

            before, after = (low_ref, high_ref) if forward else (high_ref, low_ref)
            before = ghosts(before)
            after = ghosts(after)

            def read(k):
                if k < 3:
                    return before[2 - k]
                if k >= EDGE + 3:
                    return after[k - EDGE - 3]
                c = k - 3 if forward else EDGE + 2 - k
                return in_ref[q, c, rows, lanes].astype(jnp.float32)

            def cell(k):
                return k if forward else EDGE - 1 - k

            advanced = {}
            last = None
            for f, state in faces(read, 0, 2):
                if f >= 1:
                    advanced[cell(f - 1)] = read(f + 2) - rate * (state - last)
                last = state
            advanced[cell(2)] = read(5) - rate * (mid_ref[q, 0, rows, lanes] - last)
            last = mid_ref[q, EDGE - 4, rows, lanes]
            for f, state in faces(read, EDGE - 1, EDGE):
                advanced[cell(f - 1)] = read(f + 2) - rate * (state - last)
                last = state
            for k in range(3, EDGE - 2):
                advanced[cell(k)] = mid_ref[q, k - 2, rows, lanes]
            for c in range(EDGE):
                value = advanced[c]
                if c % 2 == 1:
                    guess = advanced[c - 1]
                    if c < EDGE - 1:
                        guess = 0.5 * (guess + advanced[c + 1])
                    detail = value - guess
                    value = guess + detail - jnp.clip(detail, -limit, limit)
                work[pl.ds(c, GROUP, stride=PITCH), :] = value
            for p in range(GROUP):
                cells = work[p * PITCH : p * PITCH + EDGE, :]
                cells = jnp.where(base + p < count, cells, 0.0)
                done[q, base + p, :, lanes] = cells.astype(jnp.bfloat16)

        tiles(tile)

    def copy(q):
        return pltpu.make_async_copy(done.at[q], out_ref.at[:, q], sems.at[q])

    def quantity(q, carry):
        by_direction(speed_ref, q, run)
        copy(q).start()
        return carry

    lax.fori_loop(0, QUANT, quantity, 0)
    for q in range(QUANT):
        copy(q).wait()


PARAMS = pltpu.CompilerParams(vmem_limit_bytes=24 << 20)


def far(value):
    return pltpu.with_memory_space_constraint(value, pltpu.HBM)


def near(value):
    return pltpu.with_memory_space_constraint(value, pltpu.VMEM)


def struct(shape, dtype):
    return jax.ShapeDtypeStruct(shape, dtype)


def body(blocks, levels, destinations, speeds, thresholds):
    owners = lax.axis_size("dev")
    count = lax.axis_size("node")
    up = [(i, i + 1) for i in range(count - 1)]
    down = [(i + 1, i) for i in range(count - 1)]
    row = (owners, ROW_TILES, 8, LANES)
    outgoing = pl.pallas_call(
        pack_kernel,
        in_specs=[SMEM, SMEM, ANY],
        out_specs=ANY,
        out_shape=pltpu.HBM(row, jnp.bfloat16),
        scratch_shapes=[
            pltpu.VMEM((SLOTS, HALF_TILES, 8, PLANE), jnp.bfloat16),
            pltpu.VMEM((owners, 8, LANES), jnp.bfloat16),
            pltpu.SemaphoreType.DMA((SLOTS,)),
            pltpu.SemaphoreType.DMA((SLOTS, HALVES)),
            pltpu.SemaphoreType.DMA,
        ],
        compiler_params=PARAMS,
        name="pack",
    )(far(destinations), far(levels), far(blocks.reshape(SLOTS, HALF_TILES, 8, PLANE)))
    incoming = lax.all_to_all(outgoing, "dev", split_axis=0, concat_axis=0, tiled=True)
    sent = struct((SENT * QUANT + 1, NEW_CAP, PLANE), jnp.bfloat16)
    arranged, for_below, for_above, own, total, new_levels = pl.pallas_call(
        arrange_kernel,
        in_specs=[VMEM],
        out_specs=(VMEM, VMEM, VMEM, VMEM, SMEM, SMEM),
        out_shape=(
            pltpu.VMEM((QUANT, EDGE, NEW_CAP, PLANE), jnp.bfloat16),
            sent,
            sent,
            pltpu.VMEM((NEW_CAP, LANES), jnp.int32),
            struct((1,), jnp.int32),
            struct((NEW_CAP,), jnp.int32),
        ),
        scratch_shapes=[
            pltpu.VMEM((HALVES, NEW_CAP * PITCH + 8, LANES), jnp.float32),
            pltpu.SMEM((NEW_CAP,), jnp.int32),
            pltpu.VMEM((owners, LANES), jnp.int32),
            pltpu.SMEM((owners, LANES), jnp.int32),
            pltpu.SemaphoreType.DMA,
        ],
        compiler_params=PARAMS,
        name="arrange",
    )(near(incoming))
    ghost_high = lax.ppermute(for_below, "node", down)
    ghost_low = lax.ppermute(for_above, "node", up)
    inner = pl.pallas_call(
        inner_kernel,
        in_specs=[SMEM, VMEM],
        out_specs=VMEM,
        out_shape=pltpu.VMEM((QUANT, EDGE - 3, NEW_CAP, PLANE), jnp.float32),
        compiler_params=PARAMS,
        cost_estimate=pl.CostEstimate(
            flops=40 * QUANT * EDGE * NEW_CAP * PLANE, transcendentals=0, bytes_accessed=0
        ),
        name="inner",
    )(speeds, near(arranged))
    updated = pl.pallas_call(
        outer_kernel,
        in_specs=[SMEM, SMEM, SMEM, VMEM, VMEM, VMEM, VMEM, VMEM],
        out_specs=ANY,
        out_shape=struct((NEW_CAP, QUANT, EDGE, PLANE), jnp.bfloat16),
        scratch_shapes=[
            pltpu.VMEM((QUANT, NEW_CAP, EDGE, PLANE), jnp.bfloat16),
            pltpu.VMEM((GROUP * PITCH + 8, LANES), jnp.float32),
            pltpu.SemaphoreType.DMA((QUANT,)),
        ],
        compiler_params=PARAMS,
        name="outer",
    )(
        speeds, thresholds, total, near(own), near(arranged), near(inner),
        near(ghost_low), near(ghost_high),
    )
    return (
        updated.reshape(1, 1, NEW_CAP, QUANT, EDGE, PLANE),
        new_levels.reshape(1, 1, NEW_CAP),
    )


def solution(mesh):
    return jax.shard_map(
        body,
        mesh=mesh,
        in_specs=(
            P("node", "dev", None, None, None, None),
            P("node", "dev", None),
            P("node", "dev", None),
            P(),
            P(),
        ),
        out_specs=(P("node", "dev", None, None, None, None), P("node", "dev", None)),
        check_vma=False,
    )
```

```python
import functools

import jax
import jax.numpy as jnp
from jax import lax
from jax.experimental import pallas as pl
from jax.experimental.pallas import tpu as pltpu
from jax.sharding import PartitionSpec as P

QUANT = 7
EDGE = 16
PLANE = EDGE * EDGE
SLOTS = 16
NEW_CAP = 32
LANES = 128
HALVES = PLANE // LANES
PITCH = EDGE + 1
GROUP = 16
HALF_TILES = QUANT * EDGE // 8
ROW_TILES = HALVES * HALF_TILES + 1
SENT = 5

COURANT = 0.4
WENO_EPS = 1e-06

SMEM = pl.BlockSpec(memory_space=pltpu.SMEM)
VMEM = pl.BlockSpec(memory_space=pltpu.VMEM)
ANY = pl.BlockSpec(memory_space=pl.ANY)


def pack_kernel(dest_ref, level_ref, blocks_ref, out_ref, sems):
    last = ROW_TILES - 1
    out_ref[:, last] = jnp.zeros((out_ref.shape[0], 8, LANES), jnp.bfloat16)
    for s in range(SLOTS):
        tag = (level_ref[0, 0, s] + 1).astype(jnp.float32)
        out_ref[dest_ref[0, 0, s], last] = jnp.full((8, LANES), tag).astype(jnp.bfloat16)
    copies = []
    for s in range(SLOTS):
        for half in range(HALVES):
            copy = pltpu.make_async_copy(
                blocks_ref.at[s, :, :, half * LANES : (half + 1) * LANES],
                out_ref.at[dest_ref[0, 0, s], half * HALF_TILES : (half + 1) * HALF_TILES],
                sems.at[s, half],
            )
            copy.start()
            copies.append(copy)
    for copy in copies:
        copy.wait()


def rank_positions(in_ref, source, count_ref, new_ref, own_ref, tags_vm, tags_sm, sem):
    for i in range(NEW_CAP):
        tile = in_ref[i, ROW_TILES - 1].astype(jnp.float32)
        tags_vm[i : i + 1, :] = tile[0:1].astype(jnp.int32)
    copy = pltpu.make_async_copy(tags_vm, tags_sm, sem)
    copy.start()
    own_ref[...] = jnp.zeros_like(own_ref)
    for p in range(NEW_CAP):
        source[p] = 0
        new_ref[p] = -1
    copy.wait()
    count = jnp.int32(0)
    for i in range(NEW_CAP):
        tag = tags_sm[i, 0]
        here = tag > 0

        @pl.when(here)
        def _(i=i, tag=tag, count=count):
            source[count] = i
            new_ref[count] = tag - 1
            own_ref[pl.ds(count, 1), :] = tags_vm[pl.ds(i, 1), :]

        count = count + here.astype(jnp.int32)
    count_ref[0] = count
    return count


def outward(layers):
    sent = list(layers[:3])
    sent.append(0.5 * (layers[2] + layers[3]))
    sent.append(0.5 * (layers[4] + layers[5]))
    return [layer.astype(jnp.bfloat16) for layer in sent]


def arrange_kernel(
    in_ref, out_ref, link_ref, chip_ref, own_ref, count_ref, new_ref,
    work, source, tags_vm, tags_sm, sem,
):
    count = rank_positions(in_ref, source, count_ref, new_ref, own_ref, tags_vm, tags_sm, sem)
    even = lax.axis_index("node") % 2 == 0

    def quantity(q, carry):
        for half in range(HALVES):
            lanes = slice(half * LANES, (half + 1) * LANES)
            for p in range(NEW_CAP):
                for part in range(2):
                    tile = half * HALF_TILES + 2 * q + part
                    cells = in_ref[source[p], tile].astype(jnp.float32)
                    start = p * PITCH + part * 8
                    work[half, start : start + 8, :] = jnp.where(p < count, cells, 0.0)
            layers = []
            for c in range(EDGE):
                layer = work[half, pl.ds(c, NEW_CAP, stride=PITCH), :]
                out_ref[q, c, :, lanes] = layer.astype(jnp.bfloat16)
                layers.append(layer)
            bottom, top = outward(layers), outward(layers[::-1])
            for m in range(SENT):
                link_ref[SENT * q + m, :, lanes] = jnp.where(even, bottom[m], top[m])
                chip_ref[SENT * q + m, :, lanes] = jnp.where(even, top[m], bottom[m])
        return carry

    lax.fori_loop(0, QUANT, quantity, 0)
    label = own_ref[...].astype(jnp.float32).astype(jnp.bfloat16)
    for half in range(HALVES):
        lanes = slice(half * LANES, (half + 1) * LANES)
        link_ref[SENT * QUANT, :, lanes] = label
        chip_ref[SENT * QUANT, :, lanes] = label


def faces(read, first, last):
    cells, steps, bends, curves, turns = {}, {}, {}, {}, {}
    for k in range(first, last + 5):
        cells[k] = read(k)
        if k >= first + 1:
            steps[k] = cells[k] - cells[k - 1]
        if k >= first + 2:
            bends[k - 1] = 0.5 * (steps[k] - steps[k - 1])
            curves[k - 1] = (13.0 / 3.0) * (bends[k - 1] * bends[k - 1]) + WENO_EPS
        if k >= first + 3:
            turns[k - 1] = bends[k - 2] - bends[k - 1]
        if k >= first + 4:
            c = k - 2
            one = steps[c] + bends[c - 1]
            two = steps[c] + bends[c]
            three = steps[c + 1] - bends[c + 1]
            p_zero = curves[c - 1] + one * one
            p_one = curves[c] + two * two
            p_two = curves[c + 1] + three * three
            w_zero = p_one * p_two
            w_one = p_zero * p_two
            w_two = p_zero * p_one
            w_zero = w_zero * w_zero
            w_one = w_one * w_one
            w_two = 1.5 * (w_two * w_two)
            total = (w_zero + 6.0 * w_one) + (w_two + w_two)
            shift = (w_zero * turns[c] + w_two * turns[c + 1]) / total
            yield k - 4, 0.75 * (cells[c] + cells[c + 1]) + (shift - 0.5 * bends[c])


def tiles(body_of):
    def tile(index, carry):
        half = index % HALVES
        base = pl.multiple_of((index // HALVES) * GROUP, GROUP)
        body_of(base, pl.ds(base, GROUP), pl.ds(pl.multiple_of(half * LANES, LANES), LANES))
        return carry

    lax.fori_loop(0, HALVES * (NEW_CAP // GROUP), tile, 0)


def by_direction(speed_ref, q, run):
    @pl.when(speed_ref[q] >= 0.0)
    def _():
        run(q, True)

    @pl.when(speed_ref[q] < 0.0)
    def _():
        run(q, False)


def inner_kernel(speed_ref, in_ref, mid_ref):
    def run(q, forward):
        rate = (COURANT * 2.0 / 3.0) * jnp.abs(speed_ref[q])

        def tile(base, rows, lanes):
            def read(k):
                c = k - 3 if forward else EDGE + 2 - k
                return in_ref[q, c, rows, lanes].astype(jnp.float32)

            last = None
            for f, state in faces(read, 3, EDGE - 2):
                if f == 3:
                    mid_ref[q, 0, rows, lanes] = state
                else:
                    mid_ref[q, f - 3, rows, lanes] = read(f + 2) - rate * (state - last)
                last = state
            mid_ref[q, EDGE - 4, rows, lanes] = last

        tiles(tile)

    def quantity(q, carry):
        by_direction(speed_ref, q, run)
        return carry

    lax.fori_loop(0, QUANT, quantity, 0)


def outer_kernel(
    speed_ref, limit_ref, count_ref, own_ref, in_ref, mid_ref, link_ref, chip_ref, out_ref,
    done, work, sems,
):
    count = count_ref[0]
    even = lax.axis_index("node") % 2 == 0

    def run(q, forward, link_first):
        limit = limit_ref[q]
        rate = (COURANT * 2.0 / 3.0) * jnp.abs(speed_ref[q])

        def tile(base, rows, lanes):
            own = own_ref[rows, :].astype(jnp.float32)

            def ghosts(ref):
                sent = [
                    ref[SENT * q + m, rows, lanes].astype(jnp.float32) for m in range(SENT)
                ]
                mean = (0.5 * (sent[0] + sent[1])).astype(jnp.bfloat16).astype(jnp.float32)
                tag = ref[SENT * QUANT, rows, lanes].astype(jnp.float32)
                finer = tag > own
                coarser = tag < own
                return [
                    jnp.where(finer, fine, jnp.where(coarser, coarse, same))
                    for fine, coarse, same in (
                        (mean, sent[0], sent[0]),
                        (sent[3], sent[0], sent[1]),
                        (sent[4], sent[1], sent[2]),
                    )
                ]

            before, after = (link_ref, chip_ref) if link_first else (chip_ref, link_ref)
            before = ghosts(before)
            after = ghosts(after)

            def read(k):
                if k < 3:
                    return before[2 - k]
                if k >= EDGE + 3:
                    return after[k - EDGE - 3]
                c = k - 3 if forward else EDGE + 2 - k
                return in_ref[q, c, rows, lanes].astype(jnp.float32)

            def cell(k):
                return k if forward else EDGE - 1 - k

            advanced = {}
            last = None
            for f, state in faces(read, 0, 2):
                if f >= 1:
                    advanced[cell(f - 1)] = read(f + 2) - rate * (state - last)
                last = state
            advanced[cell(2)] = read(5) - rate * (mid_ref[q, 0, rows, lanes] - last)
            last = mid_ref[q, EDGE - 4, rows, lanes]
            for f, state in faces(read, EDGE - 1, EDGE):
                advanced[cell(f - 1)] = read(f + 2) - rate * (state - last)
                last = state
            for k in range(3, EDGE - 2):
                advanced[cell(k)] = mid_ref[q, k - 2, rows, lanes]
            for c in range(EDGE):
                value = advanced[c]
                if c % 2 == 1:
                    guess = advanced[c - 1]
                    if c < EDGE - 1:
                        guess = 0.5 * (guess + advanced[c + 1])
                    detail = value - guess
                    value = guess + detail - jnp.clip(detail, -limit, limit)
                work[pl.ds(c, GROUP, stride=PITCH), :] = value
            for p in range(GROUP):
                cells = work[p * PITCH : p * PITCH + EDGE, :]
                cells = jnp.where(base + p < count, cells, 0.0)
                done[q, base + p, :, lanes] = cells.astype(jnp.bfloat16)

        tiles(tile)

    def copy(q):
        return pltpu.make_async_copy(done.at[q], out_ref.at[:, q], sems.at[q])

    def quantity(q, carry):
        for link_first in (True, False):
            @pl.when((even == (speed_ref[q] >= 0.0)) == link_first)
            def _(link_first=link_first):
                by_direction(speed_ref, q, functools.partial(run, link_first=link_first))

        copy(q).start()
        return carry

    lax.fori_loop(0, QUANT, quantity, 0)
    for q in range(QUANT):
        copy(q).wait()


PARAMS = pltpu.CompilerParams(vmem_limit_bytes=24 << 20)


def far(value):
    return pltpu.with_memory_space_constraint(value, pltpu.HBM)


def near(value):
    return pltpu.with_memory_space_constraint(value, pltpu.VMEM)


def struct(shape, dtype):
    return jax.ShapeDtypeStruct(shape, dtype)


def swaps(start, count):
    lower = range(start, count - 1, 2)
    return [(i, i + 1) for i in lower] + [(i + 1, i) for i in lower]


def body(blocks, levels, destinations, speeds, thresholds):
    owners = lax.axis_size("dev")
    count = lax.axis_size("node")
    row = (owners, ROW_TILES, 8, LANES)
    outgoing = pl.pallas_call(
        pack_kernel,
        in_specs=[SMEM, SMEM, ANY],
        out_specs=VMEM,
        out_shape=pltpu.VMEM(row, jnp.bfloat16),
        scratch_shapes=[pltpu.SemaphoreType.DMA((SLOTS, HALVES))],
        compiler_params=PARAMS,
        name="pack",
    )(far(destinations), far(levels), far(blocks.reshape(SLOTS, HALF_TILES, 8, PLANE)))
    incoming = lax.all_to_all(outgoing, "dev", split_axis=0, concat_axis=0, tiled=True)
    sent = struct((SENT * QUANT + 1, NEW_CAP, PLANE), jnp.bfloat16)
    arranged, for_link, for_chip, own, total, new_levels = pl.pallas_call(
        arrange_kernel,
        in_specs=[VMEM],
        out_specs=(VMEM, VMEM, VMEM, VMEM, SMEM, SMEM),
        out_shape=(
            pltpu.VMEM((QUANT, EDGE, NEW_CAP, PLANE), jnp.bfloat16),
            sent,
            sent,
            pltpu.VMEM((NEW_CAP, LANES), jnp.int32),
            struct((1,), jnp.int32),
            struct((NEW_CAP,), jnp.int32),
        ),
        scratch_shapes=[
            pltpu.VMEM((HALVES, NEW_CAP * PITCH + 8, LANES), jnp.float32),
            pltpu.SMEM((NEW_CAP,), jnp.int32),
            pltpu.VMEM((owners, LANES), jnp.int32),
            pltpu.SMEM((owners, LANES), jnp.int32),
            pltpu.SemaphoreType.DMA,
        ],
        compiler_params=PARAMS,
        name="arrange",
    )(near(incoming))
    from_link = lax.ppermute(for_link, "node", swaps(1, count))
    from_chip = lax.ppermute(for_chip, "node", swaps(0, count))
    inner = pl.pallas_call(
        inner_kernel,
        in_specs=[SMEM, VMEM],
        out_specs=VMEM,
        out_shape=pltpu.VMEM((QUANT, EDGE - 3, NEW_CAP, PLANE), jnp.float32),
        compiler_params=PARAMS,
        cost_estimate=pl.CostEstimate(
            flops=40 * QUANT * EDGE * NEW_CAP * PLANE, transcendentals=0, bytes_accessed=0
        ),
        name="inner",
    )(speeds, near(arranged))
    updated = pl.pallas_call(
        outer_kernel,
        in_specs=[SMEM, SMEM, SMEM, VMEM, VMEM, VMEM, VMEM, VMEM],
        out_specs=ANY,
        out_shape=struct((NEW_CAP, QUANT, EDGE, PLANE), jnp.bfloat16),
        scratch_shapes=[
            pltpu.VMEM((QUANT, NEW_CAP, EDGE, PLANE), jnp.bfloat16),
            pltpu.VMEM((GROUP * PITCH + 8, LANES), jnp.float32),
            pltpu.SemaphoreType.DMA((QUANT,)),
        ],
        compiler_params=PARAMS,
        name="outer",
    )(
        speeds, thresholds, total, near(own), near(arranged), near(inner),
        near(from_link), near(from_chip),
    )
    return (
        updated.reshape(1, 1, NEW_CAP, QUANT, EDGE, PLANE),
        new_levels.reshape(1, 1, NEW_CAP),
    )


def solution(mesh):
    return jax.shard_map(
        body,
        mesh=mesh,
        in_specs=(
            P("node", "dev", None, None, None, None),
            P("node", "dev", None),
            P("node", "dev", None),
            P(),
            P(),
        ),
        out_specs=(P("node", "dev", None, None, None, None), P("node", "dev", None)),
        check_vma=False,
    )
```

```python
import functools

import jax
import jax.numpy as jnp
from jax import lax
from jax.experimental import pallas as pl
from jax.experimental.pallas import tpu as pltpu
from jax.sharding import PartitionSpec as P

QUANT = 7
EDGE = 16
PLANE = EDGE * EDGE
SLOTS = 16
NEW_CAP = 32
LANES = 128
HALVES = PLANE // LANES
PITCH = EDGE + 1
GROUP = 16
HALF_TILES = QUANT * EDGE // 8
ROW_TILES = HALVES * HALF_TILES + 1
SENT = 5

COURANT = 0.4
WENO_EPS = 1e-06

SMEM = pl.BlockSpec(memory_space=pltpu.SMEM)
VMEM = pl.BlockSpec(memory_space=pltpu.VMEM)
ANY = pl.BlockSpec(memory_space=pl.ANY)


def pack_kernel(dest_ref, level_ref, blocks_ref, out_ref, sems):
    last = ROW_TILES - 1
    out_ref[:, last] = jnp.zeros((out_ref.shape[0], 8, LANES), jnp.bfloat16)
    for s in range(SLOTS):
        tag = (level_ref[0, 0, s] + 1).astype(jnp.float32)
        out_ref[dest_ref[0, 0, s], last] = jnp.full((8, LANES), tag).astype(jnp.bfloat16)
    copies = []
    for s in range(SLOTS):
        for half in range(HALVES):
            copy = pltpu.make_async_copy(
                blocks_ref.at[s, :, :, half * LANES : (half + 1) * LANES],
                out_ref.at[dest_ref[0, 0, s], half * HALF_TILES : (half + 1) * HALF_TILES],
                sems.at[s, half],
            )
            copy.start()
            copies.append(copy)
    for copy in copies:
        copy.wait()


def rank_positions(in_ref, source, count_ref, new_ref, own_ref, tags_vm, tags_sm, sem):
    for i in range(NEW_CAP):
        tile = in_ref[i, ROW_TILES - 1].astype(jnp.float32)
        tags_vm[i : i + 1, :] = tile[0:1].astype(jnp.int32)
    copy = pltpu.make_async_copy(tags_vm, tags_sm, sem)
    copy.start()
    own_ref[...] = jnp.zeros_like(own_ref)
    for p in range(NEW_CAP):
        source[p] = 0
        new_ref[p] = -1
    copy.wait()
    count = jnp.int32(0)
    for i in range(NEW_CAP):
        tag = tags_sm[i, 0]
        here = tag > 0

        @pl.when(here)
        def _(i=i, tag=tag, count=count):
            source[count] = i
            new_ref[count] = tag - 1
            own_ref[pl.ds(count, 1), :] = tags_vm[pl.ds(i, 1), :]

        count = count + here.astype(jnp.int32)
    count_ref[0] = count
    return count


def outward(layers):
    sent = list(layers[:3])
    sent.append(0.5 * (layers[2] + layers[3]))
    sent.append(0.5 * (layers[4] + layers[5]))
    return [layer.astype(jnp.bfloat16) for layer in sent]


def arrange_kernel(
    in_ref, out_ref, link_ref, chip_ref, own_ref, count_ref, new_ref,
    work, source, tags_vm, tags_sm, sem,
):
    count = rank_positions(in_ref, source, count_ref, new_ref, own_ref, tags_vm, tags_sm, sem)
    even = lax.axis_index("node") % 2 == 0

    def gather(q, base):
        rows = pl.ds(base, GROUP)
        for half in range(HALVES):
            lanes = slice(half * LANES, (half + 1) * LANES)
            for p in range(GROUP):
                for part in range(2):
                    tile = half * HALF_TILES + 2 * q + part
                    cells = in_ref[source[base + p], tile].astype(jnp.float32)
                    start = p * PITCH + part * 8
                    work[half, start : start + 8, :] = jnp.where(base + p < count, cells, 0.0)
            layers = []
            for c in range(EDGE):
                layer = work[half, pl.ds(c, GROUP, stride=PITCH), :]
                out_ref[q, c, rows, lanes] = layer.astype(jnp.bfloat16)
                layers.append(layer)
            bottom, top = outward(layers), outward(layers[::-1])
            for m in range(SENT):
                link_ref[SENT * q + m, rows, lanes] = jnp.where(even, bottom[m], top[m])
                chip_ref[SENT * q + m, rows, lanes] = jnp.where(even, top[m], bottom[m])

    def quantity(q, carry):
        for index in range(NEW_CAP // GROUP):
            base = index * GROUP

            @pl.when(base < count)
            def _(base=base):
                gather(q, base)

            @pl.when(base >= count)
            def _(base=base):
                empty = jnp.zeros((SENT, GROUP, PLANE), jnp.bfloat16)
                for ref in (link_ref, chip_ref):
                    ref[pl.ds(SENT * q, SENT), base : base + GROUP, :] = empty

        return carry

    lax.fori_loop(0, QUANT, quantity, 0)
    label = own_ref[...].astype(jnp.float32).astype(jnp.bfloat16)
    for half in range(HALVES):
        lanes = slice(half * LANES, (half + 1) * LANES)
        link_ref[SENT * QUANT, :, lanes] = label
        chip_ref[SENT * QUANT, :, lanes] = label


def faces(read, first, last):
    cells, steps, bends, curves, turns = {}, {}, {}, {}, {}
    for k in range(first, last + 5):
        cells[k] = read(k)
        if k >= first + 1:
            steps[k] = cells[k] - cells[k - 1]
        if k >= first + 2:
            bends[k - 1] = 0.5 * (steps[k] - steps[k - 1])
            curves[k - 1] = (13.0 / 3.0) * (bends[k - 1] * bends[k - 1]) + WENO_EPS
        if k >= first + 3:
            turns[k - 1] = bends[k - 2] - bends[k - 1]
        if k >= first + 4:
            c = k - 2
            one = steps[c] + bends[c - 1]
            two = steps[c] + bends[c]
            three = steps[c + 1] - bends[c + 1]
            p_zero = curves[c - 1] + one * one
            p_one = curves[c] + two * two
            p_two = curves[c + 1] + three * three
            w_zero = p_one * p_two
            w_one = p_zero * p_two
            w_two = p_zero * p_one
            w_zero = w_zero * w_zero
            w_one = w_one * w_one
            w_two = 1.5 * (w_two * w_two)
            total = (w_zero + 6.0 * w_one) + (w_two + w_two)
            shift = (w_zero * turns[c] + w_two * turns[c + 1]) / total
            yield k - 4, 0.75 * (cells[c] + cells[c + 1]) + (shift - 0.5 * bends[c])


def tiles(count, body_of):
    def tile(index, carry):
        half = index % HALVES
        base = pl.multiple_of((index // HALVES) * GROUP, GROUP)
        body_of(base, pl.ds(base, GROUP), pl.ds(pl.multiple_of(half * LANES, LANES), LANES))
        return carry

    lax.fori_loop(0, HALVES * pl.cdiv(count, GROUP), tile, 0)


def by_direction(speed_ref, q, run):
    @pl.when(speed_ref[q] >= 0.0)
    def _():
        run(q, True)

    @pl.when(speed_ref[q] < 0.0)
    def _():
        run(q, False)


def inner_kernel(speed_ref, count_ref, in_ref, mid_ref):
    count = count_ref[0]

    def run(q, forward):
        rate = (COURANT * 2.0 / 3.0) * jnp.abs(speed_ref[q])

        def tile(base, rows, lanes):
            def read(k):
                c = k - 3 if forward else EDGE + 2 - k
                return in_ref[q, c, rows, lanes].astype(jnp.float32)

            last = None
            for f, state in faces(read, 3, EDGE - 2):
                if f == 3:
                    mid_ref[q, 0, rows, lanes] = state
                else:
                    mid_ref[q, f - 3, rows, lanes] = read(f + 2) - rate * (state - last)
                last = state
            mid_ref[q, EDGE - 4, rows, lanes] = last

        tiles(count, tile)

    def quantity(q, carry):
        by_direction(speed_ref, q, run)
        return carry

    lax.fori_loop(0, QUANT, quantity, 0)


def outer_kernel(
    speed_ref, limit_ref, count_ref, own_ref, in_ref, mid_ref, link_ref, chip_ref, out_ref,
    done, work, sems,
):
    count = count_ref[0]
    even = lax.axis_index("node") % 2 == 0

    def run(q, forward, link_first):
        limit = limit_ref[q]
        rate = (COURANT * 2.0 / 3.0) * jnp.abs(speed_ref[q])

        def tile(base, rows, lanes):
            own = own_ref[rows, :].astype(jnp.float32)

            def ghosts(ref):
                sent = [
                    ref[SENT * q + m, rows, lanes].astype(jnp.float32) for m in range(SENT)
                ]
                mean = (0.5 * (sent[0] + sent[1])).astype(jnp.bfloat16).astype(jnp.float32)
                tag = ref[SENT * QUANT, rows, lanes].astype(jnp.float32)
                finer = tag > own
                coarser = tag < own
                return [
                    jnp.where(finer, fine, jnp.where(coarser, coarse, same))
                    for fine, coarse, same in (
                        (mean, sent[0], sent[0]),
                        (sent[3], sent[0], sent[1]),
                        (sent[4], sent[1], sent[2]),
                    )
                ]

            before, after = (link_ref, chip_ref) if link_first else (chip_ref, link_ref)
            before = ghosts(before)
            after = ghosts(after)

            def read(k):
                if k < 3:
                    return before[2 - k]
                if k >= EDGE + 3:
                    return after[k - EDGE - 3]
                c = k - 3 if forward else EDGE + 2 - k
                return in_ref[q, c, rows, lanes].astype(jnp.float32)

            def cell(k):
                return k if forward else EDGE - 1 - k

            advanced = {}
            last = None
            for f, state in faces(read, 0, 2):
                if f >= 1:
                    advanced[cell(f - 1)] = read(f + 2) - rate * (state - last)
                last = state
            advanced[cell(2)] = read(5) - rate * (mid_ref[q, 0, rows, lanes] - last)
            last = mid_ref[q, EDGE - 4, rows, lanes]
            for f, state in faces(read, EDGE - 1, EDGE):
                advanced[cell(f - 1)] = read(f + 2) - rate * (state - last)
                last = state
            for k in range(3, EDGE - 2):
                advanced[cell(k)] = mid_ref[q, k - 2, rows, lanes]
            for c in range(EDGE):
                value = advanced[c]
                if c % 2 == 1:
                    guess = advanced[c - 1]
                    if c < EDGE - 1:
                        guess = 0.5 * (guess + advanced[c + 1])
                    detail = value - guess
                    value = guess + detail - jnp.clip(detail, -limit, limit)
                work[pl.ds(c, GROUP, stride=PITCH), :] = value
            for p in range(GROUP):
                cells = work[p * PITCH : p * PITCH + EDGE, :]
                cells = jnp.where(base + p < count, cells, 0.0)
                done[q, base + p, :, lanes] = cells.astype(jnp.bfloat16)

        tiles(count, tile)

    def copy(q):
        return pltpu.make_async_copy(done.at[q], out_ref.at[:, q], sems.at[q])

    def quantity(q, carry):
        for link_first in (True, False):
            @pl.when((even == (speed_ref[q] >= 0.0)) == link_first)
            def _(link_first=link_first):
                by_direction(speed_ref, q, functools.partial(run, link_first=link_first))

        for base in range(0, NEW_CAP, GROUP):
            @pl.when(base >= count)
            def _(base=base):
                done[q, base : base + GROUP] = jnp.zeros((GROUP, EDGE, PLANE), jnp.bfloat16)

        copy(q).start()
        return carry

    lax.fori_loop(0, QUANT, quantity, 0)
    for q in range(QUANT):
        copy(q).wait()


PARAMS = pltpu.CompilerParams(vmem_limit_bytes=24 << 20)


def far(value):
    return pltpu.with_memory_space_constraint(value, pltpu.HBM)


def near(value):
    return pltpu.with_memory_space_constraint(value, pltpu.VMEM)


def struct(shape, dtype):
    return jax.ShapeDtypeStruct(shape, dtype)


def swaps(start, count):
    lower = range(start, count - 1, 2)
    return [(i, i + 1) for i in lower] + [(i + 1, i) for i in lower]


def body(blocks, levels, destinations, speeds, thresholds):
    owners = lax.axis_size("dev")
    count = lax.axis_size("node")
    row = (owners, ROW_TILES, 8, LANES)
    outgoing = pl.pallas_call(
        pack_kernel,
        in_specs=[SMEM, SMEM, ANY],
        out_specs=VMEM,
        out_shape=pltpu.VMEM(row, jnp.bfloat16),
        scratch_shapes=[pltpu.SemaphoreType.DMA((SLOTS, HALVES))],
        compiler_params=PARAMS,
        name="pack",
    )(far(destinations), far(levels), far(blocks.reshape(SLOTS, HALF_TILES, 8, PLANE)))
    incoming = lax.all_to_all(outgoing, "dev", split_axis=0, concat_axis=0, tiled=True)
    sent = struct((SENT * QUANT + 1, NEW_CAP, PLANE), jnp.bfloat16)
    arranged, for_link, for_chip, own, total, new_levels = pl.pallas_call(
        arrange_kernel,
        in_specs=[VMEM],
        out_specs=(VMEM, VMEM, VMEM, VMEM, SMEM, SMEM),
        out_shape=(
            pltpu.VMEM((QUANT, EDGE, NEW_CAP, PLANE), jnp.bfloat16),
            sent,
            sent,
            pltpu.VMEM((NEW_CAP, LANES), jnp.int32),
            struct((1,), jnp.int32),
            struct((NEW_CAP,), jnp.int32),
        ),
        scratch_shapes=[
            pltpu.VMEM((HALVES, GROUP * PITCH + 8, LANES), jnp.float32),
            pltpu.SMEM((NEW_CAP,), jnp.int32),
            pltpu.VMEM((owners, LANES), jnp.int32),
            pltpu.SMEM((owners, LANES), jnp.int32),
            pltpu.SemaphoreType.DMA,
        ],
        compiler_params=PARAMS,
        name="arrange",
    )(near(incoming))
    from_link = lax.ppermute(for_link, "node", swaps(1, count))
    from_chip = lax.ppermute(for_chip, "node", swaps(0, count))
    inner = pl.pallas_call(
        inner_kernel,
        in_specs=[SMEM, SMEM, VMEM],
        out_specs=VMEM,
        out_shape=pltpu.VMEM((QUANT, EDGE - 3, NEW_CAP, PLANE), jnp.float32),
        compiler_params=PARAMS,
        cost_estimate=pl.CostEstimate(
            flops=40 * QUANT * EDGE * NEW_CAP * PLANE, transcendentals=0, bytes_accessed=0
        ),
        name="inner",
    )(speeds, total, near(arranged))
    updated = pl.pallas_call(
        outer_kernel,
        in_specs=[SMEM, SMEM, SMEM, VMEM, VMEM, VMEM, VMEM, VMEM],
        out_specs=ANY,
        out_shape=struct((NEW_CAP, QUANT, EDGE, PLANE), jnp.bfloat16),
        scratch_shapes=[
            pltpu.VMEM((QUANT, NEW_CAP, EDGE, PLANE), jnp.bfloat16),
            pltpu.VMEM((GROUP * PITCH + 8, LANES), jnp.float32),
            pltpu.SemaphoreType.DMA((QUANT,)),
        ],
        compiler_params=PARAMS,
        name="outer",
    )(
        speeds, thresholds, total, near(own), near(arranged), near(inner),
        near(from_link), near(from_chip),
    )
    return (
        updated.reshape(1, 1, NEW_CAP, QUANT, EDGE, PLANE),
        new_levels.reshape(1, 1, NEW_CAP),
    )


def solution(mesh):
    return jax.shard_map(
        body,
        mesh=mesh,
        in_specs=(
            P("node", "dev", None, None, None, None),
            P("node", "dev", None),
            P("node", "dev", None),
            P(),
            P(),
        ),
        out_specs=(P("node", "dev", None, None, None, None), P("node", "dev", None)),
        check_vma=False,
    )
```

```python
import functools

import jax
import jax.numpy as jnp
from jax import lax
from jax.experimental import pallas as pl
from jax.experimental.pallas import tpu as pltpu
from jax.sharding import PartitionSpec as P

QUANT = 7
EDGE = 16
PLANE = EDGE * EDGE
SLOTS = 16
NEW_CAP = 32
LANES = 128
HALVES = PLANE // LANES
PITCH = EDGE + 1
GROUP = 16
HALF_TILES = QUANT * EDGE // 8
ROW_TILES = HALVES * HALF_TILES + 1
SENT = 5

COURANT = 0.4
WENO_EPS = 1e-06

SMEM = pl.BlockSpec(memory_space=pltpu.SMEM)
VMEM = pl.BlockSpec(memory_space=pltpu.VMEM)
ANY = pl.BlockSpec(memory_space=pl.ANY)


def pack_kernel(dest_ref, level_ref, blocks_ref, out_ref, sems):
    last = ROW_TILES - 1
    out_ref[:, last] = jnp.zeros((out_ref.shape[0], 8, LANES), jnp.bfloat16)
    for s in range(SLOTS):
        tag = (level_ref[0, 0, s] + 1).astype(jnp.float32)
        out_ref[dest_ref[0, 0, s], last] = jnp.full((8, LANES), tag).astype(jnp.bfloat16)
    copies = []
    for s in range(SLOTS):
        for half in range(HALVES):
            copy = pltpu.make_async_copy(
                blocks_ref.at[s, :, :, half * LANES : (half + 1) * LANES],
                out_ref.at[dest_ref[0, 0, s], half * HALF_TILES : (half + 1) * HALF_TILES],
                sems.at[s, half],
            )
            copy.start()
            copies.append(copy)
    for copy in copies:
        copy.wait()


def rank_positions(in_ref, source, new_ref, own_ref, tags_vm, tags_sm, sem):
    for i in range(NEW_CAP):
        tile = in_ref[i, ROW_TILES - 1].astype(jnp.float32)
        tags_vm[i : i + 1, :] = tile[0:1].astype(jnp.int32)
    copy = pltpu.make_async_copy(tags_vm, tags_sm, sem)
    copy.start()
    own_ref[...] = jnp.zeros_like(own_ref)
    for p in range(NEW_CAP):
        source[p] = 0
        new_ref[p] = -1
    copy.wait()
    count = 0
    for i in range(NEW_CAP):
        tag = tags_sm[i, 0]
        source[count] = i
        new_ref[count] = tag - 1
        own_ref[pl.ds(count, 1), :] = tags_vm[i : i + 1, :]
        count = count + (tag > 0).astype(jnp.int32)
    return count


def occupied(own_ref):
    held = jnp.where(own_ref[...] > 0, 1.0 / LANES, 0.0)
    return jnp.sum(held).astype(jnp.int32)


def outward(layers):
    sent = list(layers[:3])
    sent.append(0.5 * (layers[2] + layers[3]))
    sent.append(0.5 * (layers[4] + layers[5]))
    return [layer.astype(jnp.bfloat16) for layer in sent]


def arrange_kernel(
    in_ref, out_ref, link_ref, chip_ref, own_ref, new_ref,
    work, source, tags_vm, tags_sm, sem,
):
    count = rank_positions(in_ref, source, new_ref, own_ref, tags_vm, tags_sm, sem)
    even = lax.axis_index("node") % 2 == 0

    def gather(q, base):
        rows = pl.ds(base, GROUP)
        for half in range(HALVES):
            lanes = slice(half * LANES, (half + 1) * LANES)
            for p in range(GROUP):
                for part in range(2):
                    tile = half * HALF_TILES + 2 * q + part
                    cells = in_ref[source[base + p], tile].astype(jnp.float32)
                    start = p * PITCH + part * 8
                    work[half, start : start + 8, :] = jnp.where(base + p < count, cells, 0.0)
            layers = []
            for c in range(EDGE):
                layer = work[half, pl.ds(c, GROUP, stride=PITCH), :]
                out_ref[q, c, rows, lanes] = layer.astype(jnp.bfloat16)
                layers.append(layer)
            bottom, top = outward(layers), outward(layers[::-1])
            for m in range(SENT):
                link_ref[SENT * q + m, rows, lanes] = jnp.where(even, bottom[m], top[m])
                chip_ref[SENT * q + m, rows, lanes] = jnp.where(even, top[m], bottom[m])

    def quantity(q, carry):
        for index in range(NEW_CAP // GROUP):
            base = index * GROUP

            @pl.when(base < count)
            def _(base=base):
                gather(q, base)

            @pl.when(base >= count)
            def _(base=base):
                empty = jnp.zeros((SENT, GROUP, PLANE), jnp.bfloat16)
                for ref in (link_ref, chip_ref):
                    ref[pl.ds(SENT * q, SENT), base : base + GROUP, :] = empty

        return carry

    lax.fori_loop(0, QUANT, quantity, 0)
    label = own_ref[...].astype(jnp.float32).astype(jnp.bfloat16)
    for half in range(HALVES):
        lanes = slice(half * LANES, (half + 1) * LANES)
        link_ref[SENT * QUANT, :, lanes] = label
        chip_ref[SENT * QUANT, :, lanes] = label


def faces(read, first, last):
    cells, steps, bends, curves, turns = {}, {}, {}, {}, {}
    for k in range(first, last + 5):
        cells[k] = read(k)
        if k >= first + 1:
            steps[k] = cells[k] - cells[k - 1]
        if k >= first + 2:
            bends[k - 1] = 0.5 * (steps[k] - steps[k - 1])
            curves[k - 1] = (13.0 / 3.0) * (bends[k - 1] * bends[k - 1]) + WENO_EPS
        if k >= first + 3:
            turns[k - 1] = bends[k - 2] - bends[k - 1]
        if k >= first + 4:
            c = k - 2
            one = steps[c] + bends[c - 1]
            two = steps[c] + bends[c]
            three = steps[c + 1] - bends[c + 1]
            p_zero = curves[c - 1] + one * one
            p_one = curves[c] + two * two
            p_two = curves[c + 1] + three * three
            w_zero = p_one * p_two
            w_one = p_zero * p_two
            w_two = p_zero * p_one
            w_zero = w_zero * w_zero
            w_one = w_one * w_one
            w_two = 1.5 * (w_two * w_two)
            total = (w_zero + 6.0 * w_one) + (w_two + w_two)
            shift = (w_zero * turns[c] + w_two * turns[c + 1]) / total
            yield k - 4, 0.75 * (cells[c] + cells[c + 1]) + (shift - 0.5 * bends[c])


def tiles(count, body_of):
    def tile(index, carry):
        half = index % HALVES
        base = pl.multiple_of((index // HALVES) * GROUP, GROUP)
        body_of(base, pl.ds(base, GROUP), pl.ds(pl.multiple_of(half * LANES, LANES), LANES))
        return carry

    lax.fori_loop(0, HALVES * pl.cdiv(count, GROUP), tile, 0)


def by_direction(speed_ref, q, run):
    @pl.when(speed_ref[q] >= 0.0)
    def _():
        run(q, True)

    @pl.when(speed_ref[q] < 0.0)
    def _():
        run(q, False)


def inner_kernel(speed_ref, own_ref, in_ref, mid_ref):
    count = occupied(own_ref)

    def run(q, forward):
        rate = (COURANT * 2.0 / 3.0) * jnp.abs(speed_ref[q])

        def tile(base, rows, lanes):
            def read(k):
                c = k - 3 if forward else EDGE + 2 - k
                return in_ref[q, c, rows, lanes].astype(jnp.float32)

            last = None
            for f, state in faces(read, 3, EDGE - 2):
                if f == 3:
                    mid_ref[q, 0, rows, lanes] = state
                else:
                    mid_ref[q, f - 3, rows, lanes] = read(f + 2) - rate * (state - last)
                last = state
            mid_ref[q, EDGE - 4, rows, lanes] = last

        tiles(count, tile)

    def quantity(q, carry):
        by_direction(speed_ref, q, run)
        return carry

    lax.fori_loop(0, QUANT, quantity, 0)


def outer_kernel(
    speed_ref, limit_ref, own_ref, in_ref, mid_ref, link_ref, chip_ref, out_ref,
    done, blank, work, sems,
):
    count = occupied(own_ref)
    even = lax.axis_index("node") % 2 == 0

    def run(q, forward, link_first):
        limit = limit_ref[q]
        rate = (COURANT * 2.0 / 3.0) * jnp.abs(speed_ref[q])

        def tile(base, rows, lanes):
            own = own_ref[rows, :].astype(jnp.float32)

            def ghosts(ref):
                sent = [
                    ref[SENT * q + m, rows, lanes].astype(jnp.float32) for m in range(SENT)
                ]
                mean = (0.5 * (sent[0] + sent[1])).astype(jnp.bfloat16).astype(jnp.float32)
                tag = ref[SENT * QUANT, rows, lanes].astype(jnp.float32)
                finer = tag > own
                coarser = tag < own
                return [
                    jnp.where(finer, fine, jnp.where(coarser, coarse, same))
                    for fine, coarse, same in (
                        (mean, sent[0], sent[0]),
                        (sent[3], sent[0], sent[1]),
                        (sent[4], sent[1], sent[2]),
                    )
                ]

            before, after = (link_ref, chip_ref) if link_first else (chip_ref, link_ref)
            before = ghosts(before)
            after = ghosts(after)

            def read(k):
                if k < 3:
                    return before[2 - k]
                if k >= EDGE + 3:
                    return after[k - EDGE - 3]
                c = k - 3 if forward else EDGE + 2 - k
                return in_ref[q, c, rows, lanes].astype(jnp.float32)

            def cell(k):
                return k if forward else EDGE - 1 - k

            advanced = {}
            last = None
            for f, state in faces(read, 0, 2):
                if f >= 1:
                    advanced[cell(f - 1)] = read(f + 2) - rate * (state - last)
                last = state
            advanced[cell(2)] = read(5) - rate * (mid_ref[q, 0, rows, lanes] - last)
            last = mid_ref[q, EDGE - 4, rows, lanes]
            for f, state in faces(read, EDGE - 1, EDGE):
                advanced[cell(f - 1)] = read(f + 2) - rate * (state - last)
                last = state
            for k in range(3, EDGE - 2):
                advanced[cell(k)] = mid_ref[q, k - 2, rows, lanes]
            for c in range(EDGE):
                value = advanced[c]
                if c % 2 == 1:
                    guess = advanced[c - 1]
                    if c < EDGE - 1:
                        guess = 0.5 * (guess + advanced[c + 1])
                    detail = value - guess
                    value = guess + detail - jnp.clip(detail, -limit, limit)
                work[pl.ds(c, GROUP, stride=PITCH), :] = value
            for p in range(GROUP):
                cells = work[p * PITCH : p * PITCH + EDGE, :]
                cells = jnp.where(base + p < count, cells, 0.0)
                done[q, base + p, :, lanes] = cells.astype(jnp.bfloat16)

        tiles(count, tile)

    groups = range(NEW_CAP // GROUP)

    def copy(q, g, held):
        rows = pl.ds(g * GROUP, GROUP)
        source = done.at[q, rows] if held else blank
        return pltpu.make_async_copy(source, out_ref.at[rows, q], sems.at[q, g])

    def each(q, held, act):
        for g in groups:
            @pl.when((g * GROUP < count) == held)
            def _(g=g):
                act(copy(q, g, held))

    blank[...] = jnp.zeros_like(blank)
    for q in range(QUANT):
        each(q, False, lambda dma: dma.start())

    def quantity(q, carry):
        for link_first in (True, False):
            @pl.when((even == (speed_ref[q] >= 0.0)) == link_first)
            def _(link_first=link_first):
                by_direction(speed_ref, q, functools.partial(run, link_first=link_first))

        each(q, True, lambda dma: dma.start())
        return carry

    lax.fori_loop(0, QUANT, quantity, 0)
    for q in range(QUANT):
        for held in (False, True):
            each(q, held, lambda dma: dma.wait())


PARAMS = pltpu.CompilerParams(vmem_limit_bytes=24 << 20)


def far(value):
    return pltpu.with_memory_space_constraint(value, pltpu.HBM)


def near(value):
    return pltpu.with_memory_space_constraint(value, pltpu.VMEM)


def struct(shape, dtype):
    return jax.ShapeDtypeStruct(shape, dtype)


def swaps(start, count):
    lower = range(start, count - 1, 2)
    return [(i, i + 1) for i in lower] + [(i + 1, i) for i in lower]


def body(blocks, levels, destinations, speeds, thresholds):
    owners = lax.axis_size("dev")
    count = lax.axis_size("node")
    row = (owners, ROW_TILES, 8, LANES)
    outgoing = pl.pallas_call(
        pack_kernel,
        in_specs=[SMEM, SMEM, ANY],
        out_specs=VMEM,
        out_shape=pltpu.VMEM(row, jnp.bfloat16),
        scratch_shapes=[pltpu.SemaphoreType.DMA((SLOTS, HALVES))],
        compiler_params=PARAMS,
        name="pack",
    )(far(destinations), far(levels), far(blocks.reshape(SLOTS, HALF_TILES, 8, PLANE)))
    incoming = lax.all_to_all(outgoing, "dev", split_axis=0, concat_axis=0, tiled=True)
    sent = struct((SENT * QUANT + 1, NEW_CAP, PLANE), jnp.bfloat16)
    arranged, for_link, for_chip, own, new_levels = pl.pallas_call(
        arrange_kernel,
        in_specs=[VMEM],
        out_specs=(VMEM, VMEM, VMEM, VMEM, SMEM),
        out_shape=(
            pltpu.VMEM((QUANT, EDGE, NEW_CAP, PLANE), jnp.bfloat16),
            sent,
            sent,
            pltpu.VMEM((NEW_CAP, LANES), jnp.int32),
            struct((NEW_CAP,), jnp.int32),
        ),
        scratch_shapes=[
            pltpu.VMEM((HALVES, GROUP * PITCH + 8, LANES), jnp.float32),
            pltpu.SMEM((NEW_CAP,), jnp.int32),
            pltpu.VMEM((owners, LANES), jnp.int32),
            pltpu.SMEM((owners, LANES), jnp.int32),
            pltpu.SemaphoreType.DMA,
        ],
        compiler_params=PARAMS,
        name="arrange",
    )(near(incoming))
    from_link = lax.ppermute(for_link, "node", swaps(1, count))
    from_chip = lax.ppermute(for_chip, "node", swaps(0, count))
    inner = pl.pallas_call(
        inner_kernel,
        in_specs=[SMEM, VMEM, VMEM],
        out_specs=VMEM,
        out_shape=pltpu.VMEM((QUANT, EDGE - 3, NEW_CAP, PLANE), jnp.float32),
        compiler_params=PARAMS,
        cost_estimate=pl.CostEstimate(
            flops=40 * QUANT * EDGE * NEW_CAP * PLANE, transcendentals=0, bytes_accessed=0
        ),
        name="inner",
    )(speeds, near(own), near(arranged))
    updated = pl.pallas_call(
        outer_kernel,
        in_specs=[SMEM, SMEM, VMEM, VMEM, VMEM, VMEM, VMEM],
        out_specs=ANY,
        out_shape=struct((NEW_CAP, QUANT, EDGE, PLANE), jnp.bfloat16),
        scratch_shapes=[
            pltpu.VMEM((QUANT, NEW_CAP, EDGE, PLANE), jnp.bfloat16),
            pltpu.VMEM((GROUP, EDGE, PLANE), jnp.bfloat16),
            pltpu.VMEM((GROUP * PITCH + 8, LANES), jnp.float32),
            pltpu.SemaphoreType.DMA((QUANT, NEW_CAP // GROUP)),
        ],
        compiler_params=PARAMS,
        name="outer",
    )(
        speeds, thresholds, near(own), near(arranged), near(inner),
        near(from_link), near(from_chip),
    )
    return (
        updated.reshape(1, 1, NEW_CAP, QUANT, EDGE, PLANE),
        new_levels.reshape(1, 1, NEW_CAP),
    )


def solution(mesh):
    return jax.shard_map(
        body,
        mesh=mesh,
        in_specs=(
            P("node", "dev", None, None, None, None),
            P("node", "dev", None),
            P("node", "dev", None),
            P(),
            P(),
        ),
        out_specs=(P("node", "dev", None, None, None, None), P("node", "dev", None)),
        check_vma=False,
    )
```

```python
import functools

import jax
import jax.numpy as jnp
from jax import lax
from jax.experimental import pallas as pl
from jax.experimental.pallas import tpu as pltpu
from jax.sharding import PartitionSpec as P

QUANT = 7
EDGE = 16
PLANE = EDGE * EDGE
SLOTS = 16
NEW_CAP = 32
LANES = 128
HALVES = PLANE // LANES
PITCH = EDGE + 1
GROUP = 16
HALF_TILES = QUANT * EDGE // 8
ROW_TILES = HALVES * HALF_TILES + 1
SENT = 5
LIMITS = 8

COURANT = 0.4
WENO_EPS = 1e-06

SMEM = pl.BlockSpec(memory_space=pltpu.SMEM)
VMEM = pl.BlockSpec(memory_space=pltpu.VMEM)
ANY = pl.BlockSpec(memory_space=pl.ANY)


def pack_kernel(
    dest_ref, level_ref, speed_ref, limit_ref, blocks_ref, out_ref, params_ref, sems
):
    last = ROW_TILES - 1
    out_ref[:, last] = jnp.zeros((out_ref.shape[0], 8, LANES), jnp.bfloat16)
    for s in range(SLOTS):
        tag = (level_ref[0, 0, s] + 1).astype(jnp.float32)
        out_ref[dest_ref[0, 0, s], last] = jnp.full((8, LANES), tag).astype(jnp.bfloat16)
    copies = []
    for s in range(SLOTS):
        for half in range(HALVES):
            copy = pltpu.make_async_copy(
                blocks_ref.at[s, :, :, half * LANES : (half + 1) * LANES],
                out_ref.at[dest_ref[0, 0, s], half * HALF_TILES : (half + 1) * HALF_TILES],
                sems.at[s, half],
            )
            copy.start()
            copies.append(copy)
    params_ref[...] = jnp.zeros_like(params_ref)
    for q in range(QUANT):
        params_ref[q : q + 1, :] = jnp.full((1, LANES), speed_ref[q])
        params_ref[LIMITS + q : LIMITS + q + 1, :] = jnp.full((1, LANES), limit_ref[q])
    for copy in copies:
        copy.wait()


def rank_positions(in_ref, source, new_ref, own_ref, tags_vm, tags_sm, sem):
    for i in range(NEW_CAP):
        tile = in_ref[i, ROW_TILES - 1].astype(jnp.float32)
        tags_vm[i : i + 1, :] = tile[0:1].astype(jnp.int32)
    copy = pltpu.make_async_copy(tags_vm, tags_sm, sem)
    copy.start()
    own_ref[...] = jnp.zeros_like(own_ref)
    for p in range(NEW_CAP):
        source[p] = 0
        new_ref[p] = -1
    copy.wait()
    count = 0
    for i in range(NEW_CAP):
        tag = tags_sm[i, 0]
        source[count] = i
        new_ref[count] = tag - 1
        own_ref[pl.ds(count, 1), :] = tags_vm[i : i + 1, :]
        count = count + (tag > 0).astype(jnp.int32)
    return count


def occupied(own_ref):
    held = jnp.where(own_ref[...] > 0, 1.0 / LANES, 0.0)
    return jnp.sum(held).astype(jnp.int32)


def outward(layers):
    sent = list(layers[:3])
    sent.append(0.5 * (layers[2] + layers[3]))
    sent.append(0.5 * (layers[4] + layers[5]))
    return [layer.astype(jnp.bfloat16) for layer in sent]


def arrange_kernel(
    in_ref, out_ref, link_ref, chip_ref, own_ref, new_ref,
    work, source, tags_vm, tags_sm, sem,
):
    count = rank_positions(in_ref, source, new_ref, own_ref, tags_vm, tags_sm, sem)
    even = lax.axis_index("node") % 2 == 0

    def gather(q, base):
        rows = pl.ds(base, GROUP)
        for half in range(HALVES):
            lanes = slice(half * LANES, (half + 1) * LANES)
            for p in range(GROUP):
                for part in range(2):
                    tile = half * HALF_TILES + 2 * q + part
                    cells = in_ref[source[base + p], tile].astype(jnp.float32)
                    start = p * PITCH + part * 8
                    work[half, start : start + 8, :] = jnp.where(base + p < count, cells, 0.0)
            layers = []
            for c in range(EDGE):
                layer = work[half, pl.ds(c, GROUP, stride=PITCH), :]
                out_ref[q, c, rows, lanes] = layer.astype(jnp.bfloat16)
                layers.append(layer)
            bottom, top = outward(layers), outward(layers[::-1])
            for m in range(SENT):
                link_ref[SENT * q + m, rows, lanes] = jnp.where(even, bottom[m], top[m])
                chip_ref[SENT * q + m, rows, lanes] = jnp.where(even, top[m], bottom[m])

    def quantity(q, carry):
        for index in range(NEW_CAP // GROUP):
            base = index * GROUP

            @pl.when(base < count)
            def _(base=base):
                gather(q, base)

            @pl.when(base >= count)
            def _(base=base):
                empty = jnp.zeros((SENT, GROUP, PLANE), jnp.bfloat16)
                for ref in (link_ref, chip_ref):
                    ref[pl.ds(SENT * q, SENT), base : base + GROUP, :] = empty

        return carry

    lax.fori_loop(0, QUANT, quantity, 0)
    label = own_ref[...].astype(jnp.float32).astype(jnp.bfloat16)
    for half in range(HALVES):
        lanes = slice(half * LANES, (half + 1) * LANES)
        link_ref[SENT * QUANT, :, lanes] = label
        chip_ref[SENT * QUANT, :, lanes] = label


def faces(read, first, last):
    cells, steps, bends, curves, turns = {}, {}, {}, {}, {}
    for k in range(first, last + 5):
        cells[k] = read(k)
        if k >= first + 1:
            steps[k] = cells[k] - cells[k - 1]
        if k >= first + 2:
            bends[k - 1] = 0.5 * (steps[k] - steps[k - 1])
            curves[k - 1] = (13.0 / 3.0) * (bends[k - 1] * bends[k - 1]) + WENO_EPS
        if k >= first + 3:
            turns[k - 1] = bends[k - 2] - bends[k - 1]
        if k >= first + 4:
            c = k - 2
            one = steps[c] + bends[c - 1]
            two = steps[c] + bends[c]
            three = steps[c + 1] - bends[c + 1]
            p_zero = curves[c - 1] + one * one
            p_one = curves[c] + two * two
            p_two = curves[c + 1] + three * three
            w_zero = p_one * p_two
            w_one = p_zero * p_two
            w_two = p_zero * p_one
            w_zero = w_zero * w_zero
            w_one = w_one * w_one
            w_two = 1.5 * (w_two * w_two)
            total = (w_zero + 6.0 * w_one) + (w_two + w_two)
            shift = (w_zero * turns[c] + w_two * turns[c + 1]) / total
            yield k - 4, 0.75 * (cells[c] + cells[c + 1]) + (shift - 0.5 * bends[c])


def tiles(count, body_of):
    def tile(index, carry):
        half = index % HALVES
        base = pl.multiple_of((index // HALVES) * GROUP, GROUP)
        body_of(base, pl.ds(base, GROUP), pl.ds(pl.multiple_of(half * LANES, LANES), LANES))
        return carry

    lax.fori_loop(0, HALVES * pl.cdiv(count, GROUP), tile, 0)


def backwards(params_ref):
    speeds = params_ref[0:LIMITS, :]
    row = lax.broadcasted_iota(jnp.int32, speeds.shape, 0)
    bit = jnp.left_shift(1, row).astype(jnp.float32) * (1.0 / LANES)
    return jnp.sum(jnp.where(speeds < 0.0, bit, 0.0)).astype(jnp.int32)


def by_direction(backward, q, run):
    @pl.when(jnp.logical_not(backward))
    def _():
        run(q, True)

    @pl.when(backward)
    def _():
        run(q, False)


def moves_back(bits, q):
    return (jnp.right_shift(bits, q) & 1) == 1


def inner_kernel(params_ref, own_ref, in_ref, mid_ref):
    count = occupied(own_ref)
    bits = backwards(params_ref)

    def run(q, forward):
        rate = (COURANT * 2.0 / 3.0) * jnp.abs(params_ref[pl.ds(q, 1), :])

        def tile(base, rows, lanes):
            def read(k):
                c = k - 3 if forward else EDGE + 2 - k
                return in_ref[q, c, rows, lanes].astype(jnp.float32)

            last = None
            for f, state in faces(read, 3, EDGE - 2):
                if f == 3:
                    mid_ref[q, 0, rows, lanes] = state
                else:
                    mid_ref[q, f - 3, rows, lanes] = read(f + 2) - rate * (state - last)
                last = state
            mid_ref[q, EDGE - 4, rows, lanes] = last

        tiles(count, tile)

    def quantity(q, carry):
        by_direction(moves_back(bits, q), q, run)
        return carry

    lax.fori_loop(0, QUANT, quantity, 0)


def outer_kernel(
    params_ref, own_ref, in_ref, mid_ref, link_ref, chip_ref, out_ref,
    done, blank, work, sems,
):
    count = occupied(own_ref)
    bits = backwards(params_ref)
    even = lax.axis_index("node") % 2 == 0

    def run(q, forward, link_first):
        limit = params_ref[pl.ds(LIMITS + q, 1), :]
        rate = (COURANT * 2.0 / 3.0) * jnp.abs(params_ref[pl.ds(q, 1), :])

        def tile(base, rows, lanes):
            own = own_ref[rows, :].astype(jnp.float32)

            def ghosts(ref):
                sent = [
                    ref[SENT * q + m, rows, lanes].astype(jnp.float32) for m in range(SENT)
                ]
                mean = (0.5 * (sent[0] + sent[1])).astype(jnp.bfloat16).astype(jnp.float32)
                tag = ref[SENT * QUANT, rows, lanes].astype(jnp.float32)
                finer = tag > own
                coarser = tag < own
                return [
                    jnp.where(finer, fine, jnp.where(coarser, coarse, same))
                    for fine, coarse, same in (
                        (mean, sent[0], sent[0]),
                        (sent[3], sent[0], sent[1]),
                        (sent[4], sent[1], sent[2]),
                    )
                ]

            before, after = (link_ref, chip_ref) if link_first else (chip_ref, link_ref)
            before = ghosts(before)
            after = ghosts(after)

            def read(k):
                if k < 3:
                    return before[2 - k]
                if k >= EDGE + 3:
                    return after[k - EDGE - 3]
                c = k - 3 if forward else EDGE + 2 - k
                return in_ref[q, c, rows, lanes].astype(jnp.float32)

            def cell(k):
                return k if forward else EDGE - 1 - k

            advanced = {}
            last = None
            for f, state in faces(read, 0, 2):
                if f >= 1:
                    advanced[cell(f - 1)] = read(f + 2) - rate * (state - last)
                last = state
            advanced[cell(2)] = read(5) - rate * (mid_ref[q, 0, rows, lanes] - last)
            last = mid_ref[q, EDGE - 4, rows, lanes]
            for f, state in faces(read, EDGE - 1, EDGE):
                advanced[cell(f - 1)] = read(f + 2) - rate * (state - last)
                last = state
            for k in range(3, EDGE - 2):
                advanced[cell(k)] = mid_ref[q, k - 2, rows, lanes]
            for c in range(EDGE):
                value = advanced[c]
                if c % 2 == 1:
                    guess = advanced[c - 1]
                    if c < EDGE - 1:
                        guess = 0.5 * (guess + advanced[c + 1])
                    detail = value - guess
                    value = guess + detail - jnp.clip(detail, -limit, limit)
                work[pl.ds(c, GROUP, stride=PITCH), :] = value
            for p in range(GROUP):
                cells = work[p * PITCH : p * PITCH + EDGE, :]
                cells = jnp.where(base + p < count, cells, 0.0)
                done[q, base + p, :, lanes] = cells.astype(jnp.bfloat16)

        tiles(count, tile)

    groups = range(NEW_CAP // GROUP)

    def copy(q, g, held):
        rows = pl.ds(g * GROUP, GROUP)
        source = done.at[q, rows] if held else blank
        return pltpu.make_async_copy(source, out_ref.at[rows, q], sems.at[q, g])

    def each(q, held, act):
        for g in groups:
            @pl.when((g * GROUP < count) == held)
            def _(g=g):
                act(copy(q, g, held))

    blank[...] = jnp.zeros_like(blank)
    for q in range(QUANT):
        each(q, False, lambda dma: dma.start())

    def quantity(q, carry):
        backward = moves_back(bits, q)
        for link_first in (True, False):
            @pl.when((even != backward) == link_first)
            def _(link_first=link_first):
                by_direction(backward, q, functools.partial(run, link_first=link_first))

        each(q, True, lambda dma: dma.start())
        return carry

    lax.fori_loop(0, QUANT, quantity, 0)
    for q in range(QUANT):
        for held in (False, True):
            each(q, held, lambda dma: dma.wait())


PARAMS = pltpu.CompilerParams(vmem_limit_bytes=24 << 20)


def far(value):
    return pltpu.with_memory_space_constraint(value, pltpu.HBM)


def near(value):
    return pltpu.with_memory_space_constraint(value, pltpu.VMEM)


def struct(shape, dtype):
    return jax.ShapeDtypeStruct(shape, dtype)


def swaps(start, count):
    lower = range(start, count - 1, 2)
    return [(i, i + 1) for i in lower] + [(i + 1, i) for i in lower]


def body(blocks, levels, destinations, speeds, thresholds):
    owners = lax.axis_size("dev")
    count = lax.axis_size("node")
    row = (owners, ROW_TILES, 8, LANES)
    outgoing, params = pl.pallas_call(
        pack_kernel,
        in_specs=[SMEM, SMEM, SMEM, SMEM, ANY],
        out_specs=(VMEM, VMEM),
        out_shape=(
            pltpu.VMEM(row, jnp.bfloat16),
            pltpu.VMEM((2 * LIMITS, LANES), jnp.float32),
        ),
        scratch_shapes=[pltpu.SemaphoreType.DMA((SLOTS, HALVES))],
        compiler_params=PARAMS,
        name="pack",
    )(
        far(destinations), far(levels), far(speeds), far(thresholds),
        far(blocks.reshape(SLOTS, HALF_TILES, 8, PLANE)),
    )
    incoming = lax.all_to_all(outgoing, "dev", split_axis=0, concat_axis=0, tiled=True)
    sent = struct((SENT * QUANT + 1, NEW_CAP, PLANE), jnp.bfloat16)
    arranged, for_link, for_chip, own, new_levels = pl.pallas_call(
        arrange_kernel,
        in_specs=[VMEM],
        out_specs=(VMEM, VMEM, VMEM, VMEM, SMEM),
        out_shape=(
            pltpu.VMEM((QUANT, EDGE, NEW_CAP, PLANE), jnp.bfloat16),
            sent,
            sent,
            pltpu.VMEM((NEW_CAP, LANES), jnp.int32),
            struct((NEW_CAP,), jnp.int32),
        ),
        scratch_shapes=[
            pltpu.VMEM((HALVES, GROUP * PITCH + 8, LANES), jnp.float32),
            pltpu.SMEM((NEW_CAP,), jnp.int32),
            pltpu.VMEM((owners, LANES), jnp.int32),
            pltpu.SMEM((owners, LANES), jnp.int32),
            pltpu.SemaphoreType.DMA,
        ],
        compiler_params=PARAMS,
        name="arrange",
    )(near(incoming))
    from_link = lax.ppermute(for_link, "node", swaps(1, count))
    from_chip = lax.ppermute(for_chip, "node", swaps(0, count))
    inner = pl.pallas_call(
        inner_kernel,
        in_specs=[VMEM, VMEM, VMEM],
        out_specs=VMEM,
        out_shape=pltpu.VMEM((QUANT, EDGE - 3, NEW_CAP, PLANE), jnp.float32),
        compiler_params=PARAMS,
        cost_estimate=pl.CostEstimate(
            flops=40 * QUANT * EDGE * NEW_CAP * PLANE, transcendentals=0, bytes_accessed=0
        ),
        name="inner",
    )(near(params), near(own), near(arranged))
    updated = pl.pallas_call(
        outer_kernel,
        in_specs=[VMEM, VMEM, VMEM, VMEM, VMEM, VMEM],
        out_specs=ANY,
        out_shape=struct((NEW_CAP, QUANT, EDGE, PLANE), jnp.bfloat16),
        scratch_shapes=[
            pltpu.VMEM((QUANT, NEW_CAP, EDGE, PLANE), jnp.bfloat16),
            pltpu.VMEM((GROUP, EDGE, PLANE), jnp.bfloat16),
            pltpu.VMEM((GROUP * PITCH + 8, LANES), jnp.float32),
            pltpu.SemaphoreType.DMA((QUANT, NEW_CAP // GROUP)),
        ],
        compiler_params=PARAMS,
        name="outer",
    )(
        near(params), near(own), near(arranged), near(inner),
        near(from_link), near(from_chip),
    )
    return (
        updated.reshape(1, 1, NEW_CAP, QUANT, EDGE, PLANE),
        new_levels.reshape(1, 1, NEW_CAP),
    )


def solution(mesh):
    return jax.shard_map(
        body,
        mesh=mesh,
        in_specs=(
            P("node", "dev", None, None, None, None),
            P("node", "dev", None),
            P("node", "dev", None),
            P(),
            P(),
        ),
        out_specs=(P("node", "dev", None, None, None, None), P("node", "dev", None)),
        check_vma=False,
    )
```
